256 devices in a mesh: pq: 32 (over z, x), hh: 8 (over y, core).
Axes of the slice: x: 4, y: 4, z: 8, core: 2. Of those that a mesh axis runs over, the one named last changes fastest.
Arguments:
- amplitudes: bfloat16 [4096, 8192], P('hh', 'pq'), may hold values from -6 to 6
- integrals: bfloat16 [4096, 8192], P('hh', 'pq'), may hold values from -0.0009765625 to 0.0009765625
- left_amps: bfloat16 [8, 4096, 4096], P(None, 'hh', 'pq'), may hold values from -6 to 6
Outputs:
- sigma_ladder: bfloat16 [8, 4096, 4096], P(None, 'hh', 'pq')
- subspace: float32 [8, 8], replicated
The draws below stay inside these ranges and needn't reach their ends.
All inputs are finite; a program needn't handle non-finite values.
Results may differ from the reference program's by a relative error of at most 0.0049.
Values may be sent and summed in bfloat16 or wider, within the bound.
A program may use at most 64 MiB of HBM per device.

```python
import math
import jax
import jax.numpy as jnp
from jax import lax

OCC_PAIRS = 4096
ROOTS = 8
CD_PAIRS = 8192
AB_PAIRS = 4096


def levels(stream_key, extent, shards, smallest, largest):
    def one(dim, blocks):
        steps = jax.random.uniform(jax.random.fold_in(jax.random.fold_in(stream_key, 6), dim), (blocks,), jnp.float32, smallest / len(shards), largest / len(shards))
        return jnp.repeat(jnp.exp(steps), extent[dim] // blocks).reshape((-1,) + (1,) * (len(extent) - dim - 1))

    level = one(*shards[0])
    for cut in shards[1:]:
        level = level * one(*cut)
    return level


def centred(rng, shape, scale, bound, pieces=(), kind=jnp.bfloat16):
    entries = jax.random.normal(rng, shape, jnp.float32) * scale
    if len(pieces) > 0:
        entries = levels(rng, shape, pieces, -0.22, 0.18) * entries
    return jnp.clip(entries, min=-bound, max=bound).astype(kind)


def setup_inputs(seed: int = 0) -> dict:
    seeds = jax.random.split(jax.random.key(seed), 4)
    amplitudes = centred(seeds[0], (OCC_PAIRS, CD_PAIRS), 1.0, 6.0, ((0, 8), (1, 32)))
    integrals = centred(seeds[1], (OCC_PAIRS, CD_PAIRS), (CD_PAIRS * OCC_PAIRS) ** -0.5, 0.0009765625, ((0, 8), (1, 32)))
    left_amps = centred(seeds[2], (ROOTS, OCC_PAIRS, AB_PAIRS), 1.0, 6.0, ((1, 8), (2, 32)))
    return dict(amplitudes=amplitudes, integrals=integrals, left_amps=left_amps)


def reference(amplitudes, integrals, left_amps):
    ladder = jnp.dot(amplitudes, integrals.T, preferred_element_type=jnp.float32).astype(jnp.bfloat16)
    ladder_trans = ladder.T

    def one_root(left_root):
        return jnp.dot(ladder_trans, left_root, preferred_element_type=jnp.float32).astype(jnp.bfloat16)
    sigma_ladder = lax.map(one_root, left_amps)
    flat_left = left_amps.reshape(ROOTS, -1)
    flat_sigma = sigma_ladder.reshape(ROOTS, -1)
    gram = jnp.dot(flat_left, flat_sigma.T, preferred_element_type=jnp.float32)
    subspace = gram * (1.0 / math.sqrt(OCC_PAIRS * AB_PAIRS))
    return (sigma_ladder, subspace)
```

```python
import functools
import math

import jax
import jax.numpy as jnp
from jax import lax
from jax.experimental import pallas as pl
from jax.experimental.pallas import tpu as pltpu
from jax.sharding import Mesh
from jax.sharding import PartitionSpec as P

MESH = pl.DeviceIdType.MESH
AXES = ("z", "x", "y", "core")
CHUNKS = 2
NT = (((1,), (1,)), ((), ()))


def messages(nz):
    far = nz // 2
    names = [("a", dx) for dx in (1, 2, 3)]
    names += [("i", sign, half) for sign in (1, -1) for half in (0, 1, 2)]
    for dx in range(4):
        names += [("t", dx, sign, kind) for sign in (1, -1) for kind in ("own", "fwd")]
        names += [("tc", dx, dy) for dy in range(4)]
    for k in range(CHUNKS):
        for sign, length in chains(k, far):
            names += [("r", k, sign, s) for s in range(1, length + 1)]
    names += [("l", sign, half) for sign in (1, -1) for half in (0, 1, 2)]
    names += [("lc", 0)] + [("lc", dy, half) for dy in (1, 2, 3) for half in (0, 1)]
    names += [("ax", sign, kind) for sign in (1, -1) for kind in ("own", "fwd")]
    names += [("az", dx, sign, s) for dx in range(4) for sign in (1, -1) for s in range(1, far + 1)]
    names += [("bz", sign, s) for sign in (1, -1) for s in range(1, far + 1)]
    names += [("bx", dz, sign, kind) for dz in range(nz) for sign in (1, -1) for kind in ("own", "fwd")]
    return {name: number for number, name in enumerate(names)}


def chains(k, far):
    return ((1, far), (-1, far - 1)) if k % 2 == 0 else ((-1, far), (1, far - 1))


def kernel(ids, nz, t2_hbm, int_hbm, left_hbm, out_ref, gram_ref,
           t2x, ints, part, rs_send, rs_recv, lad, left, acc, send_sem, recv_sem, local_sem):
    far = nz // 2
    size = {"z": nz, "x": 4, "y": 4, "core": 2}
    pos = {axis: lax.axis_index(axis) for axis in AXES}
    z, x, y, core = (pos[axis] for axis in AXES)
    quarter = t2x.shape[2]
    rows = lad.shape[2]
    a_rows = rows * 3 // 8
    a_span = (0, a_rows)
    b_span = (a_rows, rows - a_rows)

    def step(axis, offset):
        return lax.rem(pos[axis] + (offset + size[axis]), size[axis])

    def hidx(dy):
        return step("y", dy) * 2 + core

    h_me = y * 2 + core
    sent = []
    posted = set()

    def post(name, axis, offset, src, dst):
        k = ids[name]
        copy = pltpu.make_async_remote_copy(
            src_ref=src, dst_ref=dst, send_sem=send_sem.at[k], recv_sem=recv_sem.at[k],
            device_id={axis: step(axis, offset)}, device_id_type=MESH)
        copy.start()
        sent.append(copy)
        posted.add(name)

    def await_(name, dst):
        assert name in posted
        posted.remove(name)
        k = ids[name]
        pltpu.make_async_remote_copy(
            src_ref=dst, dst_ref=dst, send_sem=send_sem.at[k], recv_sem=recv_sem.at[k],
            device_id={"core": 1 - core}, device_id_type=MESH).wait_recv()

    own_t2 = pltpu.make_async_copy(
        t2_hbm.at[pl.ds(pl.multiple_of(x * quarter, quarter), quarter)], t2x.at[h_me, x], local_sem.at[0])
    own_int = pltpu.make_async_copy(int_hbm, ints.at[x], local_sem.at[1])
    own_left = pltpu.make_async_copy(left_hbm, left.at[h_me], local_sem.at[2])
    own_t2.start()
    own_int.start()
    own_left.start()

    barrier = pltpu.get_barrier_semaphore()
    near = (("x", 1), ("x", 2), ("x", 3), ("y", 1), ("y", 3), ("z", 1), ("z", -1), ("core", 1))
    for axis, offset in near:
        pl.semaphore_signal(barrier, inc=1, device_id={axis: step(axis, offset)}, device_id_type=MESH)
    pl.semaphore_wait(barrier, len(near))

    for dx in (2, 1, 3):
        to = step("x", dx)
        post(("a", dx), "x", dx,
             t2_hbm.at[pl.ds(pl.multiple_of(to * quarter, quarter), quarter)], t2x.at[h_me, x])
    half = rows // 2
    for sign in (1, -1):
        for n, part_no in enumerate((0, 1) if sign == 1 else (1, 0)):
            post(("i", sign, n), "x", sign,
                 int_hbm.at[pl.ds(part_no * half, half)], ints.at[x, pl.ds(part_no * half, half)])

    def t2_piece(dx):
        xi = step("x", dx)
        block = t2x.at[h_me, xi]
        for sign in (1, -1):
            post(("t", dx, sign, "own"), "y", sign, block, block)
        post(("tc", dx, 0), "core", 1, block, block)

    def t2_near(dx):
        xi = step("x", dx)
        for sign in (1, -1):
            block = t2x.at[hidx(-sign), xi]
            await_(("t", dx, sign, "own"), block)
            lo = 0 if sign == 1 else quarter // 2
            piece = t2x.at[hidx(-sign), xi, pl.ds(lo, quarter // 2)]
            post(("t", dx, sign, "fwd"), "y", sign, piece, piece)
            post(("tc", dx, -sign % 4), "core", 1, block, block)

    def t2_far(dx):
        xi = step("x", dx)
        for sign in (1, -1):
            lo = 0 if sign == 1 else quarter // 2
            await_(("t", dx, sign, "fwd"), t2x.at[hidx(2), xi, pl.ds(lo, quarter // 2)])
        block = t2x.at[hidx(2), xi]
        post(("tc", dx, 2), "core", 1, block, block)

    def int_near():
        for sign in (1, -1):
            part_no = 0 if sign == 1 else 1
            block = ints.at[step("x", -sign), pl.ds(part_no * half, half)]
            await_(("i", sign, 0), block)
            post(("i", sign, 2), "x", sign, block, block)

    own_t2.wait()
    t2_piece(0)
    for dx in (3, 1, 2):
        await_(("a", 4 - dx), t2x.at[h_me, step("x", dx)])
        t2_piece(dx)
    for dx in (0, 3):
        t2_near(dx)
    int_near()
    for dx in (1, 2):
        t2_near(dx)
    own_left.wait()
    root_half = left.shape[1] // 2
    for sign in (1, -1):
        for n, part_no in enumerate((0, 1) if sign == 1 else (1, 0)):
            block = left.at[h_me, pl.ds(part_no * root_half, root_half)]
            post(("l", sign, n), "y", sign, block, block)
    for dx in (0, 3, 1, 2):
        t2_far(dx)
    post(("lc", 0), "core", 1, left.at[h_me], left.at[h_me])
    own_int.wait()
    for sign in (1, -1):
        part_no = 1 if sign == 1 else 0
        await_(("i", sign, 1), ints.at[step("x", -sign), pl.ds(part_no * half, half)])
    for sign in (1, -1):
        part_no = 0 if sign == 1 else 1
        await_(("i", sign, 2), ints.at[step("x", 2), pl.ds(part_no * half, half)])
    for dx in (0, 3, 1, 2):
        for dy in range(4):
            await_(("tc", dx, dy), t2x.at[step("y", dy) * 2 + (1 - core), step("x", dx)])

    def partial(d):
        total = lax.dot_general(ints[0], t2x[d, 0], NT, preferred_element_type=jnp.float32)
        for xi in range(1, 4):
            total += lax.dot_general(ints[xi], t2x[d, xi], NT, preferred_element_type=jnp.float32)
        part[d] = total

    chunk = rows // CHUNKS

    def rs_step(k, sign, length, s):
        d = step("z", sign * (length + 1 - s))
        lane = 0 if sign == 1 else 1
        value = part[d, pl.ds(k * chunk, chunk)]
        if s > 1:
            await_(("r", k, sign, s - 1), rs_recv.at[k, lane, s - 2])
            value += rs_recv[k, lane, s - 2].astype(jnp.float32)
        rs_send[k, lane, s - 1] = value.astype(jnp.bfloat16)
        post(("r", k, sign, s), "z", sign, rs_send.at[k, lane, s - 1], rs_recv.at[k, lane, s - 1])

    partial(step("z", far))
    for k in range(CHUNKS):
        sign, length = chains(k, far)[0]
        rs_step(k, sign, length, 1)
    partial(step("z", far - 1))
    partial(step("z", 1 - far))
    for k in range(CHUNKS):
        sign, length = chains(k, far)[1]
        rs_step(k, sign, length, 1)

    def rest(i, carry):
        partial(lax.rem(z + (nz - far + 2) + i, nz))
        return carry

    lax.fori_loop(0, nz - 3, rest, 0)
    for s in range(2, far + 1):
        for which in (0, 1):
            for k in range(CHUNKS):
                sign, length = chains(k, far)[which]
                if s <= length:
                    rs_step(k, sign, length, s)
    for k in range(CHUNKS):
        value = part[z, pl.ds(k * chunk, chunk)]
        for sign, length in chains(k, far):
            lane = 0 if sign == 1 else 1
            await_(("r", k, sign, length), rs_recv.at[k, lane, length - 1])
            value += rs_recv[k, lane, length - 1].astype(jnp.float32)
        lad[z, x, pl.ds(k * chunk, chunk)] = value.astype(jnp.bfloat16)

    def cut(span, which):
        lo, count = span
        if which is None:
            return pl.ds(lo, count)
        return pl.ds(lo + which * (count // 2), count // 2)

    def lad_at(dz, dx, span, which=None):
        return lad.at[step("z", dz), step("x", dx), cut(span, which)]

    def along_x(tag, dz, span, dx_own=0):
        block = lad_at(dz, 0, span)
        for sign in (1, -1):
            post(tag + (sign, "own"), "x", sign, block, block)

    def x_near(tag, dz, span, sign):
        await_(tag + (sign, "own"), lad_at(dz, -sign, span))
        which = 0 if sign == 1 else 1
        piece = lad_at(dz, -sign, span, which)
        post(tag + (sign, "fwd"), "x", sign, piece, piece)

    def x_far(tag, dz, span):
        for sign in (1, -1):
            await_(tag + (sign, "fwd"), lad_at(dz, 2, span, 0 if sign == 1 else 1))

    def along_z(tag, dx, span):
        block = lad_at(0, dx, span)
        for sign in (1, -1):
            post(tag + (sign, 1), "z", sign, block, block)

    def z_hop(tag, dx, span, sign, s):
        which = 0 if sign == 1 else 1
        if s < far:
            await_(tag + (sign, s), lad_at(-sign * s, dx, span))
            block = lad_at(-sign * s, dx, span, which if s + 1 == far else None)
            post(tag + (sign, s + 1), "z", sign, block, block)
        else:
            await_(tag + (sign, s), lad_at(far, dx, span, which))

    def left_near():
        for sign in (1, -1):
            part_no = 0 if sign == 1 else 1
            block = left.at[hidx(-sign), pl.ds(part_no * root_half, root_half)]
            await_(("l", sign, 0), block)
            post(("l", sign, 2), "y", sign, block, block)
            post(("lc", -sign % 4, part_no), "core", 1, block, block)

    def left_second():
        for sign in (1, -1):
            part_no = 1 if sign == 1 else 0
            block = left.at[hidx(-sign), pl.ds(part_no * root_half, root_half)]
            await_(("l", sign, 1), block)
            post(("lc", -sign % 4, part_no), "core", 1, block, block)

    def left_far():
        for sign in (1, -1):
            part_no = 0 if sign == 1 else 1
            block = left.at[hidx(2), pl.ds(part_no * root_half, root_half)]
            await_(("l", sign, 2), block)
            post(("lc", 2, part_no), "core", 1, block, block)

    def left_partner():
        other = 1 - core
        await_(("lc", 0), left.at[y * 2 + other])
        for dy in (1, 3, 2):
            for part_no in (0, 1):
                await_(("lc", dy, part_no),
                       left.at[step("y", dy) * 2 + other, pl.ds(part_no * root_half, root_half)])

    def sigma_row(dz, first):
        h = step("z", dz)
        lhs = jnp.concatenate([lad[h, xi] for xi in range(4)], axis=1)

        def pair(j, carry):
            rhs = jnp.concatenate([left[h, 2 * j], left[h, 2 * j + 1]], axis=1)
            value = jnp.dot(lhs, rhs, preferred_element_type=jnp.float32)
            if first:
                acc[j] = value
            else:
                acc[j] += value
            return carry

        lax.fori_loop(0, acc.shape[0], pair, 0)

    along_z(("bz",), 0, b_span)
    along_x(("ax",), 0, a_span)
    along_z(("az", 0), 0, a_span)
    along_x(("bx", 0), 0, b_span)
    left_near()
    for r in range(1, far + 3):
        if r < far:
            for sign in (1, -1):
                z_hop(("bz",), 0, b_span, sign, r)
                dz = -sign * r
                along_x(("bx", dz % nz), dz, b_span)
        elif r == far:
            for sign in (1, -1):
                z_hop(("bz",), 0, b_span, sign, r)
            along_x(("bx", far), far, b_span)
        if r == 1:
            for sign in (1, -1):
                x_near(("ax",), 0, a_span, sign)
                along_z(("az", -sign % 4), -sign, a_span)
        if r == 2:
            x_far(("ax",), 0, a_span)
            along_z(("az", 2), 2, a_span)
        for dx in (0, 3, 1, 2):
            s = r - min(dx, 4 - dx)
            if 1 <= s <= far:
                for sign in (1, -1):
                    z_hop(("az", dx), dx, a_span, sign, s)
        for dz in sorted({(sign * (r - 1)) % nz for sign in (1, -1)}) if r - 1 <= far else ():
            for sign in (1, -1):
                x_near(("bx", dz), dz, b_span, sign)
        for dz in sorted({(sign * (r - 2)) % nz for sign in (1, -1)}) if 0 <= r - 2 <= far else ():
            x_far(("bx", dz), dz, b_span)
        if r == far - 1:
            left_second()
        if r == far:
            left_far()
        if r == far + 1:
            left_partner()
            for n, dz in enumerate(sorted({sign * q for q in range(far) for sign in (1, -1)}, key=abs)):
                sigma_row(dz, n == 0)
    sigma_row(far, False)

    roots = out_ref.shape[0]
    cols = out_ref.shape[2]

    def finish(j, carry):
        for i in range(2):
            s = 2 * j + i
            rounded = acc[j, :, i * cols:(i + 1) * cols].astype(jnp.bfloat16)
            out_ref[s] = rounded
            wide = rounded.astype(jnp.float32)
            lines = [jnp.sum(left[h_me, r].astype(jnp.float32) * wide, axis=0, keepdims=True)
                     for r in range(roots)]
            gram_ref[s] = jnp.concatenate(lines, axis=0)
        return carry

    lax.fori_loop(0, roots // 2, finish, 0)
    assert not posted
    for copy in sent:
        copy.wait_send()


def body(nz, amplitudes, integrals, left_amps):
    roots, rows, cols = left_amps.shape
    window = amplitudes.shape[1]
    quarter = rows // 4
    ids = messages(nz)
    far = nz // 2
    any_ = pl.BlockSpec(memory_space=pl.ANY)
    vmem = pl.BlockSpec(memory_space=pltpu.VMEM)
    sigma, gram = pl.pallas_call(
        functools.partial(kernel, ids, nz),
        out_shape=(
            jax.ShapeDtypeStruct((roots, rows, cols), jnp.bfloat16),
            jax.ShapeDtypeStruct((roots, roots, cols), jnp.float32),
        ),
        in_specs=[any_] * 3,
        out_specs=(vmem, vmem),
        scratch_shapes=[
            pltpu.VMEM((8, 4, quarter, window), jnp.bfloat16),
            pltpu.VMEM((4, rows, window), jnp.bfloat16),
            pltpu.VMEM((nz, rows, quarter), jnp.float32),
            pltpu.VMEM((CHUNKS, 2, far, rows // CHUNKS, quarter), jnp.bfloat16),
            pltpu.VMEM((CHUNKS, 2, far, rows // CHUNKS, quarter), jnp.bfloat16),
            pltpu.VMEM((nz, 4, rows, quarter), jnp.bfloat16),
            pltpu.VMEM((8, roots, rows, cols), jnp.bfloat16),
            pltpu.VMEM((roots // 2, rows, 2 * cols), jnp.float32),
            pltpu.SemaphoreType.DMA((len(ids),)),
            pltpu.SemaphoreType.DMA((len(ids),)),
            pltpu.SemaphoreType.DMA((3,)),
        ],
        compiler_params=pltpu.CompilerParams(
            collective_id=0, has_side_effects=True, vmem_limit_bytes=50 * 1024 * 1024),
    )(amplitudes, integrals, left_amps)
    local = jnp.sum(gram, axis=2).T
    occ = rows * 8
    factor = 1.0 / math.sqrt(occ * cols * nz * 4)
    return sigma, lax.psum(local, AXES) * factor


def solution(mesh):
    nz = mesh.devices.size // 32
    finer = Mesh(mesh.devices.reshape(nz, 4, 4, 2), AXES)
    placed = P(("y", "core"), ("z", "x"))
    wide = P(None, ("y", "core"), ("z", "x"))
    return jax.shard_map(
        functools.partial(body, nz), mesh=finer, in_specs=(placed, placed, wide), out_specs=(wide, P()), check_vma=False
    )
```

```python
import functools
import math

import jax
import jax.numpy as jnp
from jax import lax
from jax.experimental import pallas as pl
from jax.experimental.pallas import tpu as pltpu
from jax.sharding import Mesh
from jax.sharding import PartitionSpec as P

MESH = pl.DeviceIdType.MESH
AXES = ("z", "x", "y", "core")
CHUNKS = 2
NT = (((1,), (1,)), ((), ()))


def messages(nz):
    far = nz // 2
    names = [("a", dx) for dx in (1, 2, 3)]
    names += [("i", sign, half) for sign in (1, -1) for half in (0, 1, 2)]
    for dx in range(4):
        names += [("t", dx, sign, kind) for sign in (1, -1) for kind in ("own", "fwd")]
        names += [("tc", dx, dy) for dy in range(4)]
    for k in range(CHUNKS):
        for sign, length in chains(k, far):
            names += [("r", k, sign, s) for s in range(1, length + 1)]
    names += [("l", sign, half) for sign in (1, -1) for half in (0, 1, 2)]
    names += [("lc", 0)] + [("lc", dy, half) for dy in (1, 2, 3) for half in (0, 1)]
    names += [("ax", sign, kind) for sign in (1, -1) for kind in ("own", "fwd")]
    names += [("az", dx, sign, s) for dx in range(4) for sign in (1, -1) for s in range(1, far + 1)]
    names += [("bz", sign, s) for sign in (1, -1) for s in range(1, far + 1)]
    names += [("bx", dz, sign, kind) for dz in range(nz) for sign in (1, -1) for kind in ("own", "fwd")]
    names += [("gc", dy, dc) for dy in range(4) for dc in (0, 1) if dy or dc]
    names += [("gx", dx) for dx in (1, 2, 3)] + [("gz", dz) for dz in range(1, nz)]
    return {name: number for number, name in enumerate(names)}


def chains(k, far):
    return ((1, far), (-1, far - 1)) if k % 2 == 0 else ((-1, far), (1, far - 1))


def kernel(ids, nz, t2_hbm, int_hbm, left_hbm, out_ref, gram_ref,
           t2x, ints, part, rs_send, rs_recv, lad, left, acc, gram_y, gram_x, gram_z, send_sem, recv_sem, local_sem):
    far = nz // 2
    size = {"z": nz, "x": 4, "y": 4, "core": 2}
    pos = {axis: lax.axis_index(axis) for axis in AXES}
    z, x, y, core = (pos[axis] for axis in AXES)
    quarter = t2x.shape[2]
    rows = lad.shape[2]
    a_rows = rows * 3 // 8
    a_span = (0, a_rows)
    b_span = (a_rows, rows - a_rows)

    def step(axis, offset):
        return lax.rem(pos[axis] + (offset + size[axis]), size[axis])

    def hidx(dy):
        return step("y", dy) * 2 + core

    h_me = y * 2 + core
    sent = []
    posted = set()

    def post(name, axis, offset, src, dst):
        post_to(name, {axis: step(axis, offset)}, src, dst)

    def post_to(name, device, src, dst):
        k = ids[name]
        copy = pltpu.make_async_remote_copy(
            src_ref=src, dst_ref=dst, send_sem=send_sem.at[k], recv_sem=recv_sem.at[k],
            device_id=device, device_id_type=MESH)
        copy.start()
        sent.append(copy)
        posted.add(name)

    def await_(name, dst):
        assert name in posted
        posted.remove(name)
        k = ids[name]
        pltpu.make_async_remote_copy(
            src_ref=dst, dst_ref=dst, send_sem=send_sem.at[k], recv_sem=recv_sem.at[k],
            device_id={"core": 1 - core}, device_id_type=MESH).wait_recv()

    own_t2 = pltpu.make_async_copy(
        t2_hbm.at[pl.ds(pl.multiple_of(x * quarter, quarter), quarter)], t2x.at[h_me, x], local_sem.at[0])
    own_int = pltpu.make_async_copy(int_hbm, ints.at[x], local_sem.at[1])
    own_left = pltpu.make_async_copy(left_hbm, left.at[h_me], local_sem.at[2])
    own_t2.start()
    own_int.start()
    own_left.start()

    barrier = pltpu.get_barrier_semaphore()
    near = (("x", 1), ("x", 2), ("x", 3), ("y", 1), ("y", 3), ("z", 1), ("z", -1), ("core", 1))
    for axis, offset in near:
        pl.semaphore_signal(barrier, inc=1, device_id={axis: step(axis, offset)}, device_id_type=MESH)
    pl.semaphore_wait(barrier, len(near))

    for dx in (2, 1, 3):
        to = step("x", dx)
        post(("a", dx), "x", dx,
             t2_hbm.at[pl.ds(pl.multiple_of(to * quarter, quarter), quarter)], t2x.at[h_me, x])
    half = rows // 2
    for sign in (1, -1):
        for n, part_no in enumerate((0, 1) if sign == 1 else (1, 0)):
            post(("i", sign, n), "x", sign,
                 int_hbm.at[pl.ds(part_no * half, half)], ints.at[x, pl.ds(part_no * half, half)])

    def t2_piece(dx):
        xi = step("x", dx)
        block = t2x.at[h_me, xi]
        for sign in (1, -1):
            post(("t", dx, sign, "own"), "y", sign, block, block)
        post(("tc", dx, 0), "core", 1, block, block)

    def t2_near(dx):
        xi = step("x", dx)
        for sign in (1, -1):
            block = t2x.at[hidx(-sign), xi]
            await_(("t", dx, sign, "own"), block)
            lo = 0 if sign == 1 else quarter // 2
            piece = t2x.at[hidx(-sign), xi, pl.ds(lo, quarter // 2)]
            post(("t", dx, sign, "fwd"), "y", sign, piece, piece)
            post(("tc", dx, -sign % 4), "core", 1, block, block)

    def t2_far(dx):
        xi = step("x", dx)
        for sign in (1, -1):
            lo = 0 if sign == 1 else quarter // 2
            await_(("t", dx, sign, "fwd"), t2x.at[hidx(2), xi, pl.ds(lo, quarter // 2)])
        block = t2x.at[hidx(2), xi]
        post(("tc", dx, 2), "core", 1, block, block)

    def int_near():
        for sign in (1, -1):
            part_no = 0 if sign == 1 else 1
            block = ints.at[step("x", -sign), pl.ds(part_no * half, half)]
            await_(("i", sign, 0), block)
            post(("i", sign, 2), "x", sign, block, block)

    own_t2.wait()
    t2_piece(0)
    for dx in (3, 1, 2):
        await_(("a", 4 - dx), t2x.at[h_me, step("x", dx)])
        t2_piece(dx)
    for dx in (0, 3):
        t2_near(dx)
    int_near()
    for dx in (1, 2):
        t2_near(dx)
    own_left.wait()
    root_half = left.shape[1] // 2
    for sign in (1, -1):
        for n, part_no in enumerate((0, 1) if sign == 1 else (1, 0)):
            block = left.at[h_me, pl.ds(part_no * root_half, root_half)]
            post(("l", sign, n), "y", sign, block, block)
    for dx in (0, 3, 1, 2):
        t2_far(dx)
    post(("lc", 0), "core", 1, left.at[h_me], left.at[h_me])
    own_int.wait()
    for sign in (1, -1):
        part_no = 1 if sign == 1 else 0
        await_(("i", sign, 1), ints.at[step("x", -sign), pl.ds(part_no * half, half)])
    for sign in (1, -1):
        part_no = 0 if sign == 1 else 1
        await_(("i", sign, 2), ints.at[step("x", 2), pl.ds(part_no * half, half)])
    for dx in (0, 3, 1, 2):
        for dy in range(4):
            await_(("tc", dx, dy), t2x.at[step("y", dy) * 2 + (1 - core), step("x", dx)])

    def partial(d):
        total = lax.dot_general(ints[0], t2x[d, 0], NT, preferred_element_type=jnp.float32)
        for xi in range(1, 4):
            total += lax.dot_general(ints[xi], t2x[d, xi], NT, preferred_element_type=jnp.float32)
        part[d] = total

    chunk = rows // CHUNKS

    def rs_step(k, sign, length, s):
        d = step("z", sign * (length + 1 - s))
        lane = 0 if sign == 1 else 1
        value = part[d, pl.ds(k * chunk, chunk)]
        if s > 1:
            await_(("r", k, sign, s - 1), rs_recv.at[k, lane, s - 2])
            value += rs_recv[k, lane, s - 2].astype(jnp.float32)
        rs_send[k, lane, s - 1] = value.astype(jnp.bfloat16)
        post(("r", k, sign, s), "z", sign, rs_send.at[k, lane, s - 1], rs_recv.at[k, lane, s - 1])

    partial(step("z", far))
    for k in range(CHUNKS):
        sign, length = chains(k, far)[0]
        rs_step(k, sign, length, 1)
    partial(step("z", far - 1))
    partial(step("z", 1 - far))
    for k in range(CHUNKS):
        sign, length = chains(k, far)[1]
        rs_step(k, sign, length, 1)

    def rest(i, carry):
        partial(lax.rem(z + (nz - far + 2) + i, nz))
        return carry

    lax.fori_loop(0, nz - 3, rest, 0)
    for s in range(2, far + 1):
        for which in (0, 1):
            for k in range(CHUNKS):
                sign, length = chains(k, far)[which]
                if s <= length:
                    rs_step(k, sign, length, s)
    for k in range(CHUNKS):
        value = part[z, pl.ds(k * chunk, chunk)]
        for sign, length in chains(k, far):
            lane = 0 if sign == 1 else 1
            await_(("r", k, sign, length), rs_recv.at[k, lane, length - 1])
            value += rs_recv[k, lane, length - 1].astype(jnp.float32)
        lad[z, x, pl.ds(k * chunk, chunk)] = value.astype(jnp.bfloat16)

    def cut(span, which):
        lo, count = span
        if which is None:
            return pl.ds(lo, count)
        return pl.ds(lo + which * (count // 2), count // 2)

    def lad_at(dz, dx, span, which=None):
        return lad.at[step("z", dz), step("x", dx), cut(span, which)]

    def along_x(tag, dz, span, dx_own=0):
        block = lad_at(dz, 0, span)
        for sign in (1, -1):
            post(tag + (sign, "own"), "x", sign, block, block)

    def x_near(tag, dz, span, sign):
        await_(tag + (sign, "own"), lad_at(dz, -sign, span))
        which = 0 if sign == 1 else 1
        piece = lad_at(dz, -sign, span, which)
        post(tag + (sign, "fwd"), "x", sign, piece, piece)

    def x_far(tag, dz, span):
        for sign in (1, -1):
            await_(tag + (sign, "fwd"), lad_at(dz, 2, span, 0 if sign == 1 else 1))

    def along_z(tag, dx, span):
        block = lad_at(0, dx, span)
        for sign in (1, -1):
            post(tag + (sign, 1), "z", sign, block, block)

    def z_hop(tag, dx, span, sign, s):
        which = 0 if sign == 1 else 1
        if s < far:
            await_(tag + (sign, s), lad_at(-sign * s, dx, span))
            block = lad_at(-sign * s, dx, span, which if s + 1 == far else None)
            post(tag + (sign, s + 1), "z", sign, block, block)
        else:
            await_(tag + (sign, s), lad_at(far, dx, span, which))

    def left_near():
        for sign in (1, -1):
            part_no = 0 if sign == 1 else 1
            block = left.at[hidx(-sign), pl.ds(part_no * root_half, root_half)]
            await_(("l", sign, 0), block)
            post(("l", sign, 2), "y", sign, block, block)
            post(("lc", -sign % 4, part_no), "core", 1, block, block)

    def left_second():
        for sign in (1, -1):
            part_no = 1 if sign == 1 else 0
            block = left.at[hidx(-sign), pl.ds(part_no * root_half, root_half)]
            await_(("l", sign, 1), block)
            post(("lc", -sign % 4, part_no), "core", 1, block, block)

    def left_far():
        for sign in (1, -1):
            part_no = 0 if sign == 1 else 1
            block = left.at[hidx(2), pl.ds(part_no * root_half, root_half)]
            await_(("l", sign, 2), block)
            post(("lc", 2, part_no), "core", 1, block, block)

    def left_partner():
        other = 1 - core
        await_(("lc", 0), left.at[y * 2 + other])
        for dy in (1, 3, 2):
            for part_no in (0, 1):
                await_(("lc", dy, part_no),
                       left.at[step("y", dy) * 2 + other, pl.ds(part_no * root_half, root_half)])

    def sigma_row(dz, first):
        h = step("z", dz)
        lhs = jnp.concatenate([lad[h, xi] for xi in range(4)], axis=1)

        def pair(j, carry):
            rhs = jnp.concatenate([left[h, 2 * j], left[h, 2 * j + 1]], axis=1)
            value = jnp.dot(lhs, rhs, preferred_element_type=jnp.float32)
            if first:
                acc[j] = value
            else:
                acc[j] += value
            return carry

        lax.fori_loop(0, acc.shape[0], pair, 0)

    along_z(("bz",), 0, b_span)
    along_x(("ax",), 0, a_span)
    along_z(("az", 0), 0, a_span)
    along_x(("bx", 0), 0, b_span)
    left_near()
    for r in range(1, far + 3):
        if r < far:
            for sign in (1, -1):
                z_hop(("bz",), 0, b_span, sign, r)
                dz = -sign * r
                along_x(("bx", dz % nz), dz, b_span)
        elif r == far:
            for sign in (1, -1):
                z_hop(("bz",), 0, b_span, sign, r)
            along_x(("bx", far), far, b_span)
        if r == 1:
            for sign in (1, -1):
                x_near(("ax",), 0, a_span, sign)
                along_z(("az", -sign % 4), -sign, a_span)
        if r == 2:
            x_far(("ax",), 0, a_span)
            along_z(("az", 2), 2, a_span)
        for dx in (0, 3, 1, 2):
            s = r - min(dx, 4 - dx)
            if 1 <= s <= far:
                for sign in (1, -1):
                    z_hop(("az", dx), dx, a_span, sign, s)
        for dz in sorted({(sign * (r - 1)) % nz for sign in (1, -1)}) if r - 1 <= far else ():
            for sign in (1, -1):
                x_near(("bx", dz), dz, b_span, sign)
        for dz in sorted({(sign * (r - 2)) % nz for sign in (1, -1)}) if 0 <= r - 2 <= far else ():
            x_far(("bx", dz), dz, b_span)
        if r == far - 1:
            left_second()
        if r == far:
            left_far()
        if r == far + 1:
            left_partner()
            for n, dz in enumerate(sorted({sign * q for q in range(far) for sign in (1, -1)}, key=abs)):
                sigma_row(dz, n == 0)
    sigma_row(far, False)

    roots = out_ref.shape[0]
    cols = out_ref.shape[2]

    lane = lax.broadcasted_iota(jnp.int32, (roots, 128), 1)

    def finish(j, tile):
        for i in range(2):
            s = 2 * j + i
            rounded = acc[j, :, i * cols:(i + 1) * cols].astype(jnp.bfloat16)
            out_ref[s] = rounded
            wide = rounded.astype(jnp.float32)
            lines = [jnp.sum(left[h_me, r].astype(jnp.float32) * wide, axis=0, keepdims=True)
                     for r in range(roots)]
            column = jnp.sum(jnp.concatenate(lines, axis=0), axis=1, keepdims=True)
            tile = jnp.where(lane == s, column, tile)
        return tile

    tile = lax.fori_loop(0, roots // 2, finish, jnp.zeros((roots, 128), jnp.float32))

    def total(ref):
        value = ref[0]
        for n in range(1, ref.shape[0]):
            value += ref[n]
        return value

    gram_y[h_me] = tile
    pairs = [(dy, dc) for dy in (2, 1, 3, 0) for dc in (1, 0) if dy or dc]
    for dy, dc in pairs:
        post_to(("gc", dy, dc), {"y": step("y", dy), "core": step("core", dc)},
                gram_y.at[h_me], gram_y.at[h_me])
    for dy, dc in pairs:
        await_(("gc", dy, dc), gram_y.at[step("y", -dy) * 2 + step("core", -dc)])
    gram_x[x] = total(gram_y)
    for dx in (2, 1, 3):
        post(("gx", dx), "x", dx, gram_x.at[x], gram_x.at[x])
    for dx in (2, 1, 3):
        await_(("gx", dx), gram_x.at[step("x", -dx)])
    gram_z[z] = total(gram_x)
    hops = sorted(range(1, nz), key=lambda dz: -min(dz, nz - dz))
    for dz in hops:
        post(("gz", dz), "z", dz, gram_z.at[z], gram_z.at[z])
    for dz in hops:
        await_(("gz", dz), gram_z.at[step("z", -dz)])
    gram_ref[...] = total(gram_z)
    assert not posted
    for copy in sent:
        copy.wait_send()


def body(nz, amplitudes, integrals, left_amps):
    roots, rows, cols = left_amps.shape
    window = amplitudes.shape[1]
    quarter = rows // 4
    ids = messages(nz)
    far = nz // 2
    any_ = pl.BlockSpec(memory_space=pl.ANY)
    vmem = pl.BlockSpec(memory_space=pltpu.VMEM)
    sigma, gram = pl.pallas_call(
        functools.partial(kernel, ids, nz),
        out_shape=(
            jax.ShapeDtypeStruct((roots, rows, cols), jnp.bfloat16),
            jax.ShapeDtypeStruct((roots, 128), jnp.float32),
        ),
        in_specs=[any_] * 3,
        out_specs=(vmem, vmem),
        scratch_shapes=[
            pltpu.VMEM((8, 4, quarter, window), jnp.bfloat16),
            pltpu.VMEM((4, rows, window), jnp.bfloat16),
            pltpu.VMEM((nz, rows, quarter), jnp.float32),
            pltpu.VMEM((CHUNKS, 2, far, rows // CHUNKS, quarter), jnp.bfloat16),
            pltpu.VMEM((CHUNKS, 2, far, rows // CHUNKS, quarter), jnp.bfloat16),
            pltpu.VMEM((nz, 4, rows, quarter), jnp.bfloat16),
            pltpu.VMEM((8, roots, rows, cols), jnp.bfloat16),
            pltpu.VMEM((roots // 2, rows, 2 * cols), jnp.float32),
            pltpu.VMEM((8, roots, 128), jnp.float32),
            pltpu.VMEM((4, roots, 128), jnp.float32),
            pltpu.VMEM((nz, roots, 128), jnp.float32),
            pltpu.SemaphoreType.DMA((len(ids),)),
            pltpu.SemaphoreType.DMA((len(ids),)),
            pltpu.SemaphoreType.DMA((3,)),
        ],
        compiler_params=pltpu.CompilerParams(
            collective_id=0, has_side_effects=True, vmem_limit_bytes=63 * 1024 * 1024),
    )(amplitudes, integrals, left_amps)
    occ = rows * 8
    factor = 1.0 / math.sqrt(occ * cols * nz * 4)
    return sigma, gram[:, :roots] * factor


def solution(mesh):
    nz = mesh.devices.size // 32
    finer = Mesh(mesh.devices.reshape(nz, 4, 4, 2), AXES)
    placed = P(("y", "core"), ("z", "x"))
    wide = P(None, ("y", "core"), ("z", "x"))
    return jax.shard_map(
        functools.partial(body, nz), mesh=finer, in_specs=(placed, placed, wide), out_specs=(wide, P()), check_vma=False
    )
```
